32 devices in a mesh: rep: 2 (over x), dp: 16 (over y, z, core).
Axes of the slice: x: 2, y: 2, z: 4, core: 2. Of those that a mesh axis runs over, the one named last changes fastest.
Arguments:
- x: bfloat16 [32, 2048, 1024], P(('rep', 'dp')), parts along dimension 0
- dy: bfloat16 [32, 2048, 1024], P(('rep', 'dp')), parts along dimension 0
- w_gate: bfloat16 [2, 1024, 2816], P(None, 'dp')
- w_up: bfloat16 [2, 1024, 2816], P(None, 'dp')
- w_down: bfloat16 [2, 2816, 1024], P(None, 'dp')
Outputs:
- output 1: bfloat16 [32, 2048, 1024], P(('rep', 'dp')), parts along dimension 0
- output 2: bfloat16 [4, 1024, 2816], P('rep', 'dp'), parts along dimension 0
- output 3: bfloat16 [4, 1024, 2816], P('rep', 'dp'), parts along dimension 0
- output 4: bfloat16 [4, 2816, 1024], P('rep', 'dp'), parts along dimension 0
There are 2 independent parts. The reference program is written for one: setup_inputs(seed, part) draws one part's arguments, and reference() takes and returns one part's arrays. A program takes and returns all parts, laid end to end along the dimension named above; an argument that names none is the same for every part.
All inputs are finite; a program needn't handle non-finite values.
Results may differ from the reference program's by a relative error of at most 0.018.
Values are sent between devices in bfloat16 or wider.
A program may use at most 2 GiB of HBM per device.

```python
import jax
import jax.numpy as jnp
from jax import lax

SEQUENCES = 16
TOKENS = 2048
D = 1024
FF = 2816
LAYERS = 2
NAMES = ("w_gate", "w_up", "w_down")
SHAPES = {"w_gate": (LAYERS, D, FF), "w_up": (LAYERS, D, FF), "w_down": (LAYERS, FF, D)}


def bump(key, n, height):
    away = (jnp.arange(n, dtype=jnp.int32) - jax.random.randint(key, (), 0, n, jnp.int32)) % n
    return jnp.where(away < n // 8, height, 1.0)


def together(key, own, strength):
    shared = jax.random.normal(key, own.shape[1:], jnp.float32)
    return (own + strength * shared) * lax.rsqrt(1 + strength * strength)


def setup_inputs(seed: int = 0, part: int = 0) -> dict:
    kx, kdy, ka, kb, kz, kf, kh, kl, *kw = jax.random.split(jax.random.key(seed), 8 + len(NAMES))
    kx, kdy, ka, kb = (jax.random.fold_in(k, part) for k in (kx, kdy, ka, kb))
    shape = (SEQUENCES, TOKENS, D)
    much_x, much_dy = jax.random.uniform(kz, (2,), jnp.float32, 0.0, 1.0)
    layers = 2.0 ** jax.random.uniform(kl, (LAYERS, 1, 1), jnp.float32, -1.0, 1.0)
    x = together(ka, jax.random.normal(kx, shape, jnp.float32), much_x) * bump(kf, D, 4.0)
    dy = together(kb, jax.random.normal(kdy, shape, jnp.float32), much_dy)
    drawn = {"x": x.astype(jnp.bfloat16), "dy": (dy * (SEQUENCES * TOKENS) ** -0.5).astype(jnp.bfloat16)}
    for key, name in zip(kw, NAMES, strict=True):
        w = jax.random.normal(key, SHAPES[name], jnp.float32) * SHAPES[name][1] ** -0.5
        drawn[name] = (w * {"w_gate": 1.0, "w_up": bump(kh, FF, 4.0), "w_down": layers}[name]).astype(jnp.bfloat16)
    return drawn


def matmul(a, w):
    return jnp.dot(a, w, preferred_element_type=jnp.float32).astype(jnp.bfloat16)


def normed(h):
    wide = h.astype(jnp.float32)
    scale = lax.rsqrt(jnp.mean(wide**2, -1, keepdims=True) + 1e-6)
    return (wide * scale).astype(jnp.bfloat16)


def layer(h, w):
    a = normed(h)
    gate = jnp.dot(a, w["w_gate"], preferred_element_type=jnp.float32)
    up = jnp.dot(a, w["w_up"], preferred_element_type=jnp.float32)
    return h + matmul((jax.nn.silu(gate) * up).astype(jnp.bfloat16), w["w_down"])


def stack(weights, h):
    return lax.scan(lambda h, w: (layer(h, w), None), h, weights)[0]


def reference(x, dy, w_gate, w_up, w_down):
    weights = dict(zip(NAMES, (w_gate, w_up, w_down), strict=True))

    def take(so_far, sequence):
        h, by_y = sequence
        _, back = jax.vjp(stack, weights, h)
        by_weights, by_h = back(by_y)
        return jax.tree.map(lambda total, term: total + term.astype(jnp.float32), so_far, by_weights), by_h

    none_yet = {name: jnp.zeros(w.shape, jnp.float32) for name, w in weights.items()}
    by_weights, by_x = lax.scan(take, none_yet, (x, dy))
    return (by_x, *(by_weights[name].astype(jnp.bfloat16) for name in NAMES))
```

```python
import jax
import jax.numpy as jnp
from jax import lax
from jax.sharding import Mesh, PartitionSpec as P

F32, BF16 = jnp.float32, jnp.bfloat16
SWAP = [(0, 1), (1, 0)]


def dot(a, b, contract):
    return lax.dot_general(a, b, (contract, ((), ())), preferred_element_type=F32)


def normed(h):
    wide = h.astype(F32)
    scale = lax.rsqrt(jnp.mean(wide**2, -1, keepdims=True) + 1e-6)
    return (wide * scale).astype(BF16)


def swap(t):
    return lax.ppermute(t, "core", SWAP)


def solution(mesh):
    groups, size = mesh.shape["rep"], mesh.shape["dp"]
    chips = size // 2
    mine = Mesh(mesh.devices.reshape(groups, chips, 2), ("rep", "yz", "core"))

    def step(x, dy, w_gate, w_up, w_down):
        x, dy = x[0], dy[0]
        layers, rows, ff = w_gate.shape
        part = w_down.shape[1]
        half = ff // 2
        both = jnp.stack([w_gate, w_up], 1).reshape(layers * 2, rows, chips, 2, part)
        both = both.transpose(3, 0, 1, 2, 4).reshape(2, layers * 2, rows, half)
        both = lax.all_to_all(both, "core", 0, 0, tiled=True)
        both = both.transpose(1, 0, 2, 3).reshape(layers, 2, 2 * rows, half)

        def gather(t):
            own = lax.all_gather(t, "yz", tiled=True)
            return own, swap(own)

        def scatter(own, other):
            came = swap(other.astype(BF16))
            total = (own + came.astype(F32)).astype(BF16)
            return lax.psum_scatter(total, "yz", scatter_dimension=0, tiled=True)

        wg, wu, wd = [], [], []
        for l in range(layers):
            wg.append(gather(both[l, 0]))
            wu.append(gather(both[l, 1]))
            wd.append(gather(w_down[l]))

        h = x
        hs, saved = [], []
        for l in range(layers):
            a = normed(h)
            gate = [dot(a, w, ((1,), (0,))) for w in wg[l]]
            up = [dot(a, w, ((1,), (0,))) for w in wu[l]]
            act = [(jax.nn.silu(g) * u).astype(BF16) for g, u in zip(gate, up)]
            hs.append(h)
            saved.append((a, gate, up, act))
            if l < layers - 1:
                out = dot(act[0], wd[l][0], ((1,), (0,))) + dot(act[1], wd[l][1], ((1,), (0,)))
                h = h + out.astype(BF16)

        dh = dy
        grads = [None] * layers
        for l in reversed(range(layers)):
            a, gate, up, act = saved[l]
            d_down = scatter(*(dot(t, dh, ((0,), (0,))) for t in act))
            d_gate, d_up = [], []
            for g, u, w in zip(gate, up, wd[l]):
                d_act = dot(dh, w, ((1,), (1,))).astype(BF16).astype(F32)
                sig = jax.nn.sigmoid(g)
                d_gate.append((d_act * u * (sig * (1 + g * (1 - sig)))).astype(BF16))
                d_up.append((d_act * (g * sig)).astype(BF16))
            g_gate = scatter(*(dot(a, t, ((0,), (0,))) for t in d_gate))
            g_up = scatter(*(dot(a, t, ((0,), (0,))) for t in d_up))
            da = sum(dot(t, w, ((1,), (1,))) for t, w in zip(d_gate + d_up, wg[l] + wu[l]))
            da = da.astype(BF16).astype(F32)
            wide = hs[l].astype(F32)
            inv = lax.rsqrt(jnp.mean(wide**2, -1, keepdims=True) + 1e-6)
            proj = jnp.mean(da * wide, -1, keepdims=True) * (inv * inv * inv)
            dh = (dh.astype(F32) + (da * inv - wide * proj).astype(BF16).astype(F32)).astype(BF16)
            grads[l] = (g_gate, g_up, d_down)

        pair = jnp.stack([jnp.stack(g[:2]) for g in grads])
        pair = pair.reshape(layers * 2, 2, rows, half).transpose(1, 0, 2, 3)
        pair = lax.all_to_all(pair, "core", 0, 0, tiled=True)
        pair = pair.reshape(2, layers, 2, rows, chips, part).transpose(1, 2, 3, 4, 0, 5).reshape(layers, 2, rows, ff)
        return dh[None], pair[:, 0], pair[:, 1], jnp.stack([g[2] for g in grads])

    device = ("yz", "core")
    weight = P(None, device, None)
    seq = P(("rep",) + device, None, None)
    grad = P("rep", device, None)
    return jax.shard_map(
        step, mesh=mine, in_specs=(seq, seq, weight, weight, weight), out_specs=(seq, grad, grad, grad), check_vma=False
    )
```

```python
import functools

import jax
import jax.numpy as jnp
from jax import lax
from jax.experimental import pallas as pl
from jax.experimental.pallas import tpu as pltpu
from jax.sharding import Mesh, PartitionSpec as P


F32, BF16 = jnp.float32, jnp.bfloat16
SWAP = [(0, 1), (1, 0)]
CHIPS = 8
ANY = pl.BlockSpec(memory_space=pl.ANY)


def dot(a, b, ca, cb):
    return lax.dot_general(a, b, (((ca,), (cb,)), ((), ())), preferred_element_type=F32)


def at(q):
    q = q % CHIPS
    return jnp.where(q < CHIPS // 2, q, CHIPS + CHIPS // 2 - 1 - q)


def place(q):
    q = q % CHIPS
    return q if q < CHIPS // 2 else CHIPS + CHIPS // 2 - 1 - q


RIGHT = [(place(q), place(q + 1)) for q in range(CHIPS)]
LEFT = [(place(q + 1), place(q)) for q in range(CHIPS)]
STEPS = {False: (4, 3), True: (3, 4)}


def offsets(flip):
    left, right = STEPS[flip]
    return [0] + [-j for j in range(1, left + 1)] + [j for j in range(1, right + 1)]


class Gather:
    def __init__(self, piece, flip):
        self.way = [[piece], [piece]]
        self.flip = flip
        self.sib = {}
        self.swap()

    def swap(self):
        for i, way in enumerate(self.way):
            for j in range(min(i, 1), len(way)):
                if (i, j) not in self.sib:
                    self.sib[i, j] = lax.ppermute(way[j], "core", SWAP)

    def step(self):
        old = [len(w) for w in self.way]
        for i, (steps, to) in enumerate(zip(STEPS[self.flip], (RIGHT, LEFT))):
            if old[i] <= steps:
                self.way[i].append(lax.ppermute(self.way[i][-1], "yz", to))

    def pieces(self):
        keys = [(0, j) for j in range(len(self.way[0]))] + [(1, j) for j in range(1, len(self.way[1]))]
        return [self.way[i][j] for i, j in keys], [self.sib[key] for key in keys]


class Scatter:
    def __init__(self, terms, p, flip):
        self.terms, self.p = lax.optimization_barrier((terms, p))
        self.left = list(STEPS[flip])
        self.came = [None, None]

    def step(self):
        for i, (way, sign) in enumerate(((RIGHT, 1), (LEFT, -1))):
            j = self.left[i]
            if j:
                p, came, terms = self.p, self.came[i], self.terms
                if came is not None:
                    p, came, terms = lax.optimization_barrier((p, came, terms))
                send = lax.dynamic_index_in_dim(terms, at(p + sign * j + CHIPS), 0, False)
                if came is not None:
                    send = send + came.astype(F32)
                self.came[i] = lax.ppermute(send.astype(BF16), "yz", way)
                self.left[i] -= 1

    def result(self):
        assert self.left == [0, 0]
        p, terms, *came = lax.optimization_barrier((self.p, self.terms, *self.came))
        total = lax.dynamic_index_in_dim(terms, at(p), 0, False)
        for t in came:
            total = total + t.astype(F32)
        return total.astype(BF16)


def cost(flops, *arrays):
    return pl.CostEstimate(
        flops=int(flops), bytes_accessed=int(sum(a.size * a.dtype.itemsize for a in arrays)), transcendentals=0
    )


class Weight:
    def __init__(self, pieces, shape):
        self.own, self.sib = pieces
        self.shape = shape

    @property
    def operands(self):
        return [*self.own, *self.sib]

    def copies(self, refs, meta, table, whole, sem):
        c = meta[0]
        out = []
        rows, half = refs[0].shape[1:]
        for number, ref in enumerate(refs):
            side = c if number < CHIPS else 1 - c
            chip = meta[1 + table * CHIPS + number % CHIPS]
            col = pl.multiple_of(side * half, 128)
            for k in range(2):
                core = side if k == 0 else 1 - side
                row = pl.multiple_of((2 * chip + core) * rows, 16)
                out.append(pltpu.make_async_copy(ref.at[k], whole.at[pl.ds(row, rows), pl.ds(col, half)], sem))
        return out


def with_weights(body, weights, tables, meta, grid, in_specs, ins, out_specs, out_shape, scratch, flops, prior=()):
    n_in, n_out = len(ins), len(out_shape)

    def kernel(meta_ref, *refs):
        at_in, refs = refs[:n_in], refs[n_in:]
        at_w = []
        for _ in weights:
            at_w.append(refs[: 2 * CHIPS])
            refs = refs[2 * CHIPS :]
        refs = refs[len(prior) :]
        outs, refs = refs[:n_out], refs[n_out:]
        wholes, refs = refs[: len(weights)], refs[len(weights) :]
        sem, rest = refs[0], refs[1:]
        first = functools.reduce(jnp.logical_and, [pl.program_id(i) == 0 for i in range(len(grid))])

        @pl.when(first)
        def _():
            copies = []
            for w, r, whole, table in zip(weights, at_w, wholes, tables):
                copies += w.copies(r, meta_ref, table, whole, sem)
            for t in copies:
                t.start()
            for t in copies:
                t.wait()

        body(at_in, outs, wholes, rest)

    operands = [t for w in weights for t in w.operands]
    return pl.pallas_call(
        kernel,
        out_shape=out_shape,
        grid_spec=pltpu.PrefetchScalarGridSpec(
            num_scalar_prefetch=1,
            grid=grid,
            in_specs=list(in_specs) + [ANY] * (len(operands) + len(prior)),
            out_specs=out_specs,
            scratch_shapes=[pltpu.VMEM(w.shape, BF16) for w in weights] + [pltpu.SemaphoreType.DMA] + list(scratch),
        ),
        cost_estimate=cost(flops, *ins, *operands, *out_shape),
        input_output_aliases={1 + n_in + len(operands) + i: i for i in range(len(prior))},
        compiler_params=pltpu.CompilerParams(dimension_semantics=("arbitrary",) * len(grid)),
    )(meta, *ins, *operands, *prior)


def solution(mesh):
    groups, size = mesh.shape["rep"], mesh.shape["dp"]
    mine = Mesh(mesh.devices.reshape(groups, size // 2, 2), ("rep", "yz", "core"))

    def step(x, dy, w_gate, w_up, w_down):
        x, dy = x[0], dy[0]
        layers, rows, ff = w_gate.shape
        tokens, d = x.shape
        fh, dh_ = ff // 2, d // 2
        c = lax.axis_index("core")
        k = lax.axis_index("yz")
        p = jnp.where(k < CHIPS // 2, k, CHIPS + CHIPS // 2 - 1 - k)
        meta = jnp.stack([c] + [at(p + o + CHIPS) for f in (False, True) for o in offsets(f)]).astype(jnp.int32)

        both = jnp.stack([w_gate, w_up], 1).reshape(layers * 2, rows, ff)
        take = lambda t, side, n: lax.dynamic_slice_in_dim(t, side * n, n, -1)
        gu = jnp.stack([take(both, c, fh), lax.ppermute(take(both, 1 - c, fh), "core", SWAP)], 1)
        dn = jnp.stack([take(w_down, c, dh_), lax.ppermute(take(w_down, 1 - c, dh_), "core", SWAP)], 1)
        gathers = {}
        for l in range(layers):
            gathers.update({f"g{l}": Gather(gu[2 * l], False), f"u{l}": Gather(gu[2 * l + 1], True), f"d{l}": Gather(dn[l], bool(l))})

        wg, wu, wd = [None] * 2, [None] * 2, [None] * 2

        tm = tokens // 2
        tn = 256
        tile = lambda r, n, o=0: pl.BlockSpec((r, n), lambda i, *_: (i + o, 0))
        cell = lambda o=0: pl.BlockSpec((tm, tn), lambda i, j, *_: (i + o, j))
        one = 2 * tokens * d * ff

        def normed(wide):
            return (wide * lax.rsqrt(jnp.mean(wide * wide, -1, keepdims=True) + 1e-6)).astype(BF16)

        def columns():
            return pl.ds(pl.multiple_of(pl.program_id(1) * tn, tn), tn)

        def gate_up(a, l, part, prior):
            def body(ins, outs, ws, _):
                n = columns()
                g = dot(ins[0][...], ws[0][:, n], 1, 0)
                u = dot(ins[0][...], ws[1][:, n], 1, 0)
                outs[0][...] = g
                outs[1][...] = u
                outs[2][...] = (g * jax.nn.sigmoid(g) * u).astype(BF16)

            shape = lambda t: jax.ShapeDtypeStruct((tokens, ff), t)
            return with_weights(
                body, [wg[l], wu[l]], [0, 1], meta, (1, ff // tn), [tile(tm, d, part)], [a],
                [cell(part)] * 3, [shape(F32), shape(F32), shape(BF16)], [], one, prior,
            )

        def d_gate_up(d_act, g, u):
            sig = jax.nn.sigmoid(g)
            return (d_act * u * (sig * (1 + g * (1 - sig)))).astype(BF16), (d_act * (g * sig)).astype(BF16)

        def last(a, d_act, l):
            def body(ins, outs, ws, _):
                n = columns()
                g = dot(ins[0][...], ws[0][:, n], 1, 0)
                u = dot(ins[0][...], ws[1][:, n], 1, 0)
                d_act = ins[1][...].astype(F32)
                outs[0][...] = (g * jax.nn.sigmoid(g) * u).astype(BF16)
                outs[1][...], outs[2][...] = d_gate_up(d_act, g, u)

            return with_weights(
                body, [wg[l], wu[l]], [0, 1], meta, (tokens // tm, ff // tn), [tile(tm, d), cell()], [a, d_act],
                [cell()] * 3, [jax.ShapeDtypeStruct((tokens, ff), BF16)] * 3, [], 2 * one,
            )

        def d_act_of(dh, l):
            def body(ins, outs, ws, _):
                outs[0][...] = dot(ins[0][...], ws[0][columns(), :], 1, 1).astype(BF16)

            return with_weights(
                body, [wd[l]], [l], meta, (tokens // tm, ff // tn), [tile(tm, d)], [dh],
                [cell()], [jax.ShapeDtypeStruct((tokens, ff), BF16)], [], one,
            )[0]

        def d_hidden(dh, gate, up, l):
            def body(ins, outs, ws, _):
                d_act = dot(ins[0][...], ws[0][columns(), :], 1, 1).astype(BF16).astype(F32)
                outs[0][...], outs[1][...] = d_gate_up(d_act, ins[1][...], ins[2][...])

            return with_weights(
                body, [wd[l]], [l], meta, (tokens // tm, ff // tn), [tile(tm, d), cell(), cell()], [dh, gate, up],
                [cell()] * 2, [jax.ShapeDtypeStruct((tokens, ff), BF16)] * 2, [], one,
            )

        tt = tokens // 4

        def down(act, h, l):
            def body(ins, outs, ws, _):
                out = dot(ins[0][...], ws[0][...], 1, 0).astype(BF16)
                new = (ins[1][...].astype(F32) + out.astype(F32)).astype(BF16)
                outs[0][...] = new
                outs[1][...] = normed(new.astype(F32))

            return with_weights(
                body, [wd[l]], [l], meta, (tokens // tt,), [tile(tt, ff), tile(tt, d)], [act, h],
                [tile(tt, d)] * 2, [jax.ShapeDtypeStruct((tokens, d), BF16)] * 2, [], one,
            )

        def back(d_gate, d_up, h, dh, l, part, prior):
            def body(ins, outs, ws, _):
                da = dot(ins[0][...], ws[0][...], 1, 1) + dot(ins[1][...], ws[1][...], 1, 1)
                da = da.astype(BF16).astype(F32)
                wide = ins[2][...].astype(F32)
                inv = lax.rsqrt(jnp.mean(wide * wide, -1, keepdims=True) + 1e-6)
                proj = jnp.mean(da * wide, -1, keepdims=True) * (inv * inv * inv)
                term = (da * inv - wide * proj).astype(BF16).astype(F32)
                outs[0][...] = (ins[3][...].astype(F32) + term).astype(BF16)

            return with_weights(
                body, [wg[l], wu[l]], [0, 1], meta, (2,), [tile(tt, ff, 2 * part)] * 2 + [tile(tt, d, 2 * part)] * 2,
                [d_gate, d_up, h, dh], [tile(tt, d, 2 * part)], [jax.ShapeDtypeStruct((tokens, d), BF16)], [], one, prior,
            )

        def outer(a, b, came):
            m, half = a.shape[1], b.shape[1] // 2
            tk = min(512, tokens)
            steps = tokens // tk
            own = came is not None

            def kernel(meta_ref, a_ref, b_ref, *refs):
                i = pl.program_id(0)
                if own:
                    came_ref, out, got, sem = refs
                    acc = out
                    copy = pltpu.make_async_copy(came_ref, got, sem)

                    @pl.when(i == 0)
                    def _():
                        copy.start()
                else:
                    out, acc = refs
                t = dot(a_ref[...], b_ref[...], 0, 0)

                @pl.when(i == 0)
                def _():
                    acc[...] = t

                @pl.when(i > 0)
                def _():
                    acc[...] += t

                @pl.when(i == steps - 1)
                def _():
                    if own:
                        copy.wait()
                        out[...] += got[...].astype(F32)
                    else:
                        out[...] = acc[...].astype(BF16)

            whole = pl.BlockSpec((m, half), lambda i, meta: (0, 0))
            side = (lambda meta: meta[0]) if own else (lambda meta: 1 - meta[0])
            out = jax.ShapeDtypeStruct((m, half), F32 if own else BF16)
            extra = [came] if own else []
            return pl.pallas_call(
                kernel,
                out_shape=out,
                grid_spec=pltpu.PrefetchScalarGridSpec(
                    num_scalar_prefetch=1,
                    grid=(steps,),
                    in_specs=[
                        pl.BlockSpec((tk, m), lambda i, meta: (i, 0)),
                        pl.BlockSpec((tk, half), lambda i, meta: (i, side(meta))),
                    ] + [ANY] * len(extra),
                    out_specs=whole,
                    scratch_shapes=[pltpu.VMEM((m, half), BF16), pltpu.SemaphoreType.DMA] if own else [pltpu.VMEM((m, half), F32)],
                ),
                cost_estimate=cost(one // 2, a, out, *extra, *extra),
                compiler_params=pltpu.CompilerParams(dimension_semantics=("arbitrary",)),
            )(meta, a, b, *extra)

        def keep(total):
            t = total.reshape(2, -1, total.shape[-1])
            here = lax.dynamic_index_in_dim(t, c, 0, False)
            came = lax.ppermute(lax.dynamic_index_in_dim(t, 1 - c, 0, False), "core", SWAP)
            return jnp.concatenate([jnp.where(c == 0, here, came), jnp.where(c == 0, came, here)], -1)

        rings = dict(gathers)

        def slot(names, work):
            for name in names.split():
                rings[name].step()
            return work() if work else None

        def gathered(l, *names):
            for name in names:
                gathers[name].swap()
                shape = (ff, d) if name[0] == "d" else (d, ff)
                {"g": wg, "u": wu, "d": wd}[name[0]][l] = Weight(gathers[name].pieces(), shape)

        def move(*names):
            for name in names:
                gathers[name].swap()

        def send(half):
            return lax.ppermute(half, "core", SWAP)

        def ring(name, own, flip):
            rings[name] = Scatter(own.reshape(CHIPS, -1, own.shape[-1]), p, flip)

        h0 = x
        a0 = normed(x.astype(F32))
        for _ in range(4):
            slot("g0 u0", None)
            move("g0", "u0")
        gathered(0, "g0", "u0")
        first = slot("d0 d1", lambda: gate_up(a0, 0, 0, ()))
        move("d0", "d1")
        gate0, up0, act0 = slot("d0 d1", lambda: gate_up(a0, 0, 1, first))
        for _ in range(2):
            move("d0", "d1")
            slot("d0 d1", None)
        gathered(0, "d0")
        gathered(1, "d1")
        h1, a1 = slot("g1 u1", lambda: down(act0, h0, 0))
        move("g1", "u1")
        d_act1 = slot("g1 u1", lambda: d_act_of(dy, 1))
        for _ in range(2):
            move("g1", "u1")
            slot("g1 u1", None)
        gathered(1, "g1", "u1")
        act1, dg1, du1 = last(a1, d_act1, 1)

        d1s = send(outer(act1, dy, None))
        g1s = send(outer(a1, dg1, None))
        ring("d1", outer(act1, dy, d1s), False)
        g1, u1s = slot("d1", lambda: (outer(a1, dg1, g1s), send(outer(a1, du1, None))))
        ring("g1", g1, True)
        first, u1 = slot("d1 g1", lambda: (back(dg1, du1, h1, dy, 1, 0, ()), outer(a1, du1, u1s)))
        ring("u1", u1, False)
        (dh1,) = slot("d1 g1 u1", lambda: back(dg1, du1, h1, dy, 1, 1, first))
        d0s, dg0, du0 = slot("d1 g1 u1", lambda: (send(outer(act0, dh1, None)), *d_hidden(dh1, gate0, up0, 0)))
        d0, g0s = slot("g1 u1", lambda: (outer(act0, dh1, d0s), send(outer(a0, dg0, None))))
        ring("d0", d0, True)
        g0, u0s = slot("u1 d0", lambda: (outer(a0, dg0, g0s), send(outer(a0, du0, None))))
        ring("g0", g0, False)
        u0 = slot("d0 g0", lambda: outer(a0, du0, u0s))
        ring("u0", u0, True)
        first = slot("d0 g0 u0", lambda: back(dg0, du0, h0, dh1, 0, 0, ()))
        (dx,) = slot("d0 g0 u0", lambda: back(dg0, du0, h0, dh1, 0, 1, first))
        slot("g0 u0", None)
        slot("u0", None)
        done = {name: keep(r.result()) for name, r in rings.items()}
        out = [jnp.stack([done[n + "0"], done[n + "1"]]) for n in "gud"]
        return dx[None], *out

    device = ("yz", "core")
    weight = P(None, device, None)
    seq = P(("rep",) + device, None, None)
    grad = P("rep", device, None)
    return jax.shard_map(
        step, mesh=mine, in_specs=(seq, seq, weight, weight, weight), out_specs=(seq, grad, grad, grad), check_vma=False
    )
```
